256 devices in a mesh: batch: 4 (over x, y), rows: 64 (over z, core).
Axes of the slice: x: 2, y: 2, z: 32, core: 2. Of those that a mesh axis runs over, the one named last changes fastest.
The devices are a block of a 4x8x32 slice.
Arguments:
- latent: bfloat16 [16, 1536, 256], P(None, ('batch', 'rows')), parts along dimension 1, may hold values from -11 to 11
- kernel_in: bfloat16 [3, 3, 16, 512], replicated, may hold values from -0.5 to 0.5
- gain_one: float32 [512], replicated, may hold values from 0.25 to 1.75
- bias_one: float32 [512], replicated, may hold values from -3 to 3
- kernel_one: bfloat16 [3, 3, 512, 512], replicated, may hold values from -0.09375 to 0.09375
- gain_two: float32 [512], replicated, may hold values from 0.25 to 1.75
- bias_two: float32 [512], replicated, may hold values from -3 to 3
- kernel_two: bfloat16 [3, 3, 512, 512], replicated, may hold values from -0.09375 to 0.09375
Outputs:
- block_out: bfloat16 [1536, 256, 512], P(('batch', 'rows')), parts along dimension 0
The draws below stay inside these ranges and needn't reach their ends.
There are 4 independent parts, one for each index of `batch`. The reference program is written for one: setup_inputs(seed, part) draws one part's arguments, and reference() takes and returns one part's arrays. A program takes and returns all parts, laid end to end along the dimension named above; an argument that names none is the same for every part. Nothing has to cross between parts.
All inputs are finite; a program needn't handle non-finite values.
Results may differ from the reference program's by a relative error of at most 0.014.
Values may be sent and summed in bfloat16 or wider, within the bound.
No kernel may reach another device: no remote copies, remote signals or barrier semaphores. Data moves between devices by JAX's collectives and lax.ppermute only.
A program may use at most 64 MiB of HBM per device.

```python
import jax
import jax.numpy as jnp
from jax import lax

C = 512
GROUPS = 32
LC = 16
COLS = 256
HEIGHT = 384


def draw_latent(key, part):
    keys = jax.random.split(jax.random.fold_in(key, 11), 7)
    heights = jnp.arange(HEIGHT, dtype=jnp.float32) / (HEIGHT - 1)
    direction = (2 * jax.random.randint(keys[0], (), 0, 2) - 1).astype(jnp.float32)
    trend = direction * 0.9 * (2.0 * heights - 1.0)
    rough = jax.random.uniform(keys[1], (HEIGHT,), jnp.float32, -0.3, 0.3)
    switch = jax.random.uniform(keys[2], (), jnp.float32, 0.3, 0.7)
    side = jnp.where(heights < switch, -1.0, 1.0)
    level = jax.random.uniform(keys[3], (LC, 1, 1), jnp.float32, -0.3, 0.3)
    offset = level * side[None, :, None] + jax.random.uniform(keys[4], (LC, HEIGHT, 1), jnp.float32, -0.1, 0.1)
    row_ids = jnp.arange(HEIGHT, dtype=jnp.int32)
    col_ids = jnp.arange(COLS, dtype=jnp.int32)
    row_edge = (row_ids == 0) | (row_ids == HEIGHT - 1)
    col_edge = (col_ids == 0) | (col_ids == COLS - 1)
    border = row_edge[:, None] | col_edge[None, :]
    inner_scale = 0.2 * jnp.exp(trend + rough)
    outer_scale = 4.5 * jnp.exp(0.5 * trend + rough)
    outer_noise = jax.random.uniform(keys[6], (LC, HEIGHT, COLS), jnp.float32, -1.0, 1.0)
    noise = jnp.clip(jax.random.normal(keys[5], (LC, HEIGHT, COLS), jnp.float32), -4.0, 4.0)
    inner = noise * inner_scale[None, :, None]
    outer = outer_noise * outer_scale[None, :, None]
    values = offset + jnp.where(border[None, :, :], outer, inner)
    return values.astype(jnp.bfloat16)


def normal_values(own_key, dims, scale, limit, held_as=jnp.bfloat16):
    return jnp.clip(scale * jax.random.normal(own_key, dims, jnp.float32), -limit, limit).astype(held_as)


def setup_inputs(seed: int = 0, part: int = 0) -> dict:
    streams_of = jax.random.split(jax.random.key(seed), 9)
    own_keys = jax.random.split(jax.random.fold_in(streams_of[8], part), 9)
    return {
        "latent": draw_latent(jax.random.fold_in(jax.random.fold_in(streams_of[8], part), 71), part),
        "kernel_in": normal_values(streams_of[1], (3, 3, LC, C), (9 * LC) ** -0.5, 0.5),
        "gain_one": jnp.clip(1.0 + 0.15 * jax.random.normal(streams_of[2], (C,), jnp.float32), 0.25, 1.75),
        "bias_one": normal_values(streams_of[3], (C,), 0.5, 3.0, jnp.float32),
        "kernel_one": normal_values(streams_of[4], (3, 3, C, C), (9 * C) ** -0.5, 0.09375),
        "gain_two": jnp.clip(1.0 + 0.15 * jax.random.normal(streams_of[5], (C,), jnp.float32), 0.25, 1.75),
        "bias_two": normal_values(streams_of[6], (C,), 0.5, 3.0, jnp.float32),
        "kernel_two": normal_values(streams_of[7], (3, 3, C, C), (9 * C) ** -0.5, 0.09375),
    }


EPSILON = 1e-06

def convolve(padded, kernel):
    height = padded.shape[0] - 2
    width = padded.shape[1] - 2
    inputs = padded.shape[2]
    total = jnp.zeros((height * width, kernel.shape[3]), jnp.float32)
    for row_shift in range(3):
        band = padded[row_shift:row_shift + height]
        stacked = jnp.concatenate([band[:, col_shift:col_shift + width] for col_shift in range(3)], axis=-1)
        total = total + jnp.dot(stacked.reshape(height * width, 3 * inputs).astype(jnp.float32), kernel[row_shift].reshape(3 * inputs, -1).astype(jnp.float32), preferred_element_type=jnp.float32)
    return total.reshape(height, width, -1)

def pad_cells(field):
    return jnp.pad(field, ((1, 1), (1, 1), (0, 0)))

def group_activate(field, gain, bias):
    values = field.astype(jnp.float32).reshape(field.shape[0], field.shape[1], GROUPS, -1)
    center = lax.optimization_barrier(jnp.mean(values, axis=(0, 1, 3)))
    spread = lax.optimization_barrier(jnp.mean((values - center[None, None, :, None]) ** 2, axis=(0, 1, 3)))
    normed = (values - center[None, None, :, None]) * lax.rsqrt(spread + EPSILON)[None, None, :, None]
    normed = normed.reshape(field.shape) * gain + bias
    return jax.nn.silu(normed).astype(jnp.bfloat16)

def reference(latent, kernel_in, gain_one, bias_one, kernel_one, gain_two, bias_two, kernel_two):
    image = jnp.transpose(latent, (1, 2, 0))
    features = convolve(pad_cells(image), kernel_in).astype(jnp.bfloat16)
    first = group_activate(features, gain_one, bias_one)
    hidden = convolve(pad_cells(first), kernel_one).astype(jnp.bfloat16)
    second = group_activate(hidden, gain_two, bias_two)
    result = features.astype(jnp.float32) + convolve(pad_cells(second), kernel_two)
    return result.astype(jnp.bfloat16)
```

```python
import jax
import jax.numpy as jnp
from jax import lax
from jax.experimental import pallas as pl
from jax.experimental.pallas import tpu as pltpu
from jax.sharding import PartitionSpec as P

GROUPS = 32
EPSILON = 1e-06
LANES = 128
HALO = 3
EXACT = lax.Precision.HIGHEST


def dot(a, b):
    return jnp.dot(a, b, preferred_element_type=jnp.float32)


def member(channels, offset, transposed):
    shape = (LANES, channels) if transposed else (channels, LANES)
    channel = lax.broadcasted_iota(jnp.int32, shape, 1 if transposed else 0)
    lane = lax.broadcasted_iota(jnp.int32, shape, 0 if transposed else 1)
    return (channel // (channels // GROUPS) + offset == lane).astype(jnp.float32)


def store_moments(out_ref, sums, squares):
    channels = sums.shape[-1]
    line = jnp.dot(
        jnp.broadcast_to(sums, (8, channels)), member(channels, 0, False), precision=EXACT, preferred_element_type=jnp.float32
    ) + jnp.dot(
        jnp.broadcast_to(squares, (8, channels)), member(channels, GROUPS, False), precision=EXACT, preferred_element_type=jnp.float32
    )
    for at in range(0, out_ref.shape[0], 8):
        out_ref[pl.ds(at, 8), :] = line


def half_affine(all_ref, gain_ref, bias_ref, cells):
    channels = gain_ref.shape[-1]
    count = cells * (channels // GROUPS) * all_ref.shape[0]
    means = jnp.sum(all_ref[...], axis=0, keepdims=True) / count
    means = jnp.broadcast_to(means, (8, LANES))
    center = jnp.dot(means, member(channels, 0, True), precision=EXACT, preferred_element_type=jnp.float32)
    square = jnp.dot(means, member(channels, GROUPS, True), precision=EXACT, preferred_element_type=jnp.float32)
    spread = jnp.maximum(square - center * center, 0.0)
    scale = lax.rsqrt(spread + EPSILON)[0:1] * gain_ref[...]
    shift = bias_ref[...] - center[0:1] * scale
    return scale * 0.5, shift * 0.5


def activate_row(value, scale, shift, inside, x_ref, slot):
    cols, channels = value.shape
    half = value.astype(jnp.float32) * scale + shift
    act = half * jnp.tanh(half) + half
    if inside is not None:
        act = jnp.where(inside, act, 0.0)
    zero = jnp.zeros((1, channels), jnp.float32)
    rows = pl.ds(slot * cols, cols)
    x_ref[rows, 0:channels] = jnp.concatenate([zero, act[:-1]], axis=0).astype(jnp.bfloat16)
    x_ref[rows, channels : 2 * channels] = act.astype(jnp.bfloat16)
    x_ref[rows, 2 * channels :] = jnp.concatenate([act[1:], zero], axis=0).astype(jnp.bfloat16)


def conv_row(x_ref, slot, weight_ref, cols):
    parts = [x_ref[pl.ds((slot + a) * cols, cols), :] for a in range(3)]
    return dot(jnp.concatenate(parts, axis=1), weight_ref[...])


def fill_patches(patch_ref, at, row):
    inputs, cols = row.shape
    values = row.astype(jnp.float32)
    lane = lax.broadcasted_iota(jnp.int32, values.shape, 1)
    left = jnp.where(lane == 0, 0.0, pltpu.roll(values, 1, 1))
    right = jnp.where(lane == cols - 1, 0.0, pltpu.roll(values, cols - 1, 1))
    for b, moved in enumerate((left, values, right)):
        patch_ref[pl.ds((3 * at + b) * inputs, inputs), :] = moved.astype(jnp.bfloat16)


def feature_row(patch_ref, at, inputs, weight):
    patch = patch_ref[pl.ds(3 * at * inputs, 9 * inputs), :]
    return lax.dot_general(patch, weight, (((0,), (0,)), ((), ())), preferred_element_type=jnp.float32).astype(jnp.bfloat16)


def feature_rows(patch_ref, spots, inputs, weight, out_ref):
    sums = squares = 0.0
    for r, at in enumerate(spots):
        rounded = feature_row(patch_ref, at, inputs, weight)
        out_ref[r] = rounded
        values = rounded.astype(jnp.float32)
        sums = sums + jnp.sum(values, axis=0, keepdims=True)
        squares = squares + jnp.sum(values * values, axis=0, keepdims=True)
    return sums, squares


def inner_features(own_ref, weight_ref, out_ref, sums_ref, patch_ref):
    rows, inputs, _ = own_ref.shape
    for at in range(rows):
        fill_patches(patch_ref, at, own_ref[at])
    sums, squares = feature_rows(patch_ref, range(rows - 2), inputs, weight_ref[...], out_ref)
    sums_ref[0:1, :] = sums
    sums_ref[1:2, :] = squares


def outer_features(prev_ref, own_ref, next_ref, weight_ref, sums_ref, out_ref, moments_ref, patch_ref):
    rows, inputs, _ = own_ref.shape
    lines = [prev_ref[HALO - 1], own_ref[0], own_ref[1], own_ref[rows - 2], own_ref[rows - 1], next_ref[0]]
    for at, line in enumerate(lines):
        fill_patches(patch_ref, at, line)
    sums, squares = feature_rows(patch_ref, (0, 3), inputs, weight_ref[...], out_ref)
    store_moments(moments_ref, sums + sums_ref[0:1, :], squares + sums_ref[1:2, :])


def halo_features(prev_ref, own_ref, next_ref, weight_ref, out_ref, patch_ref):
    rows, inputs, _ = own_ref.shape
    lines = [prev_ref[r] for r in range(3)] + [own_ref[0], own_ref[rows - 1]] + [next_ref[r] for r in range(3)]
    for at, line in enumerate(lines):
        fill_patches(patch_ref, at, line)
    weight = weight_ref[...]
    for r, at in enumerate((0, 1, 4, 5)):
        out_ref[r] = feature_row(patch_ref, at, inputs, weight)


def weight_copies(source_ref, weight_ref, sems):
    depth = weight_ref.shape[0] // 3
    return [
        pltpu.make_async_copy(source_ref.at[pl.ds(a * depth, depth)], weight_ref.at[pl.ds(a * depth, depth)], sems.at[a])
        for a in range(3)
    ]


def first_conv_row(x_ref, slot, weight_ref, cols, copies):
    depth = weight_ref.shape[0] // 3
    total = 0.0
    for a, copy in enumerate(copies):
        copy.wait()
        total = total + dot(x_ref[pl.ds((slot + a) * cols, cols), :], weight_ref[pl.ds(a * depth, depth), :])
    return total


def feature_at(inner_ref, outer_ref, r):
    last = inner_ref.shape[0] + 1
    return outer_ref[r // last] if r in (0, last) else inner_ref[r - 1]


def own_hidden(
    edge_ref, inner_ref, outer_ref, halo_ref, all_ref, gain_ref, bias_ref, source_ref, out_ref, moments_ref,
    x_ref, weight_ref, stage_ref, weight_sems, sems,
):
    rows, cols = inner_ref.shape[0] + 2, inner_ref.shape[1]
    weights = weight_copies(source_ref, weight_ref, weight_sems)
    for copy in weights:
        copy.start()
    scale, shift = half_affine(all_ref, gain_ref, bias_ref, rows * cols)
    sums = squares = 0.0

    def fill(slot):
        if slot == 0:
            activate_row(halo_ref[1], scale, shift, edge_ref[0] > 0, x_ref, slot)
        elif slot == rows + 1:
            activate_row(halo_ref[2], scale, shift, edge_ref[1] > 0, x_ref, slot)
        else:
            activate_row(feature_at(inner_ref, outer_ref, slot - 1), scale, shift, None, x_ref, slot)

    for slot in range(3):
        fill(slot)
    copies = []
    for r in range(rows):
        if r:
            fill(r + 2)
        total = conv_row(x_ref, r, weight_ref, cols) if r else first_conv_row(x_ref, r, weight_ref, cols, weights)
        rounded = total.astype(jnp.bfloat16)
        stage_ref[r] = rounded
        copies.append(pltpu.make_async_copy(stage_ref.at[r], out_ref.at[r], sems.at[r]))
        copies[-1].start()
        values = rounded.astype(jnp.float32)
        sums = sums + jnp.sum(values, axis=0, keepdims=True)
        squares = squares + jnp.sum(values * values, axis=0, keepdims=True)
    store_moments(moments_ref, sums, squares)
    for copy in copies:
        copy.wait()


def halo_hidden(
    edge_ref, inner_ref, outer_ref, halo_ref, all_ref, gain_ref, bias_ref, source_ref, out_ref, x_ref, weight_ref, weight_sems
):
    rows, cols = inner_ref.shape[0] + 2, inner_ref.shape[1]
    weights = weight_copies(source_ref, weight_ref, weight_sems)
    for copy in weights:
        copy.start()
    scale, shift = half_affine(all_ref, gain_ref, bias_ref, rows * cols)
    above, below = edge_ref[0] > 0, edge_ref[1] > 0
    activate_row(halo_ref[0], scale, shift, above, x_ref, 0)
    activate_row(halo_ref[1], scale, shift, above, x_ref, 1)
    activate_row(outer_ref[0], scale, shift, None, x_ref, 2)
    out_ref[0] = first_conv_row(x_ref, 0, weight_ref, cols, weights).astype(jnp.bfloat16)
    activate_row(outer_ref[1], scale, shift, None, x_ref, 3)
    activate_row(halo_ref[2], scale, shift, below, x_ref, 4)
    activate_row(halo_ref[3], scale, shift, below, x_ref, 5)
    out_ref[1] = conv_row(x_ref, 3, weight_ref, cols).astype(jnp.bfloat16)


def residual(
    edge_ref, hidden_ref, halo_ref, inner_ref, outer_ref, all_ref, gain_ref, bias_ref, source_ref, out_ref,
    x_ref, weight_ref, own_ref, stage_ref, weight_sems, own_sems, sems,
):
    rows, cols = inner_ref.shape[0] + 2, inner_ref.shape[1]
    loads = [pltpu.make_async_copy(hidden_ref.at[r], own_ref.at[r], own_sems.at[r]) for r in range(rows)]
    weights = weight_copies(source_ref, weight_ref, weight_sems)
    for copy in loads[:2] + weights + loads[2:]:
        copy.start()
    scale, shift = half_affine(all_ref, gain_ref, bias_ref, rows * cols)

    def fill(slot):
        if slot == 0:
            activate_row(halo_ref[0], scale, shift, edge_ref[0] > 0, x_ref, slot)
        elif slot == rows + 1:
            activate_row(halo_ref[1], scale, shift, edge_ref[1] > 0, x_ref, slot)
        else:
            activate_row(own_ref[slot - 1], scale, shift, None, x_ref, slot)

    loads[0].wait()
    loads[1].wait()
    for slot in range(3):
        fill(slot)
    copies = []
    for r in range(rows):
        if r == 1:
            for copy in loads[2:]:
                copy.wait()
        if r:
            fill(r + 2)
        total = conv_row(x_ref, r, weight_ref, cols) if r else first_conv_row(x_ref, r, weight_ref, cols, weights)
        total = feature_at(inner_ref, outer_ref, r).astype(jnp.float32) + total
        stage_ref[r] = total.astype(jnp.bfloat16)
        copies.append(pltpu.make_async_copy(stage_ref.at[r], out_ref.at[r], sems.at[r]))
        copies[-1].start()
    for copy in copies:
        copy.wait()


def call(body, outs, scratch, operands, flops, limit, specs=None, out_specs=None):
    vmem = pl.BlockSpec(memory_space=pltpu.VMEM)
    return pl.pallas_call(
        body,
        out_shape=outs,
        in_specs=specs or [vmem] * len(operands),
        out_specs=out_specs or jax.tree.map(lambda _: vmem, outs),
        scratch_shapes=scratch,
        cost_estimate=pl.CostEstimate(flops=flops, transcendentals=0, bytes_accessed=1 << 20),
        compiler_params=pltpu.CompilerParams(vmem_limit_bytes=limit << 20),
    )(*operands)


def over_all(moments, axis):
    spread = lax.all_to_all(moments[:, None, :], axis, split_axis=0, concat_axis=0, tiled=True)
    return spread[:, 0, :]


def local(latent, kernel_in, gain_one, bias_one, kernel_one, gain_two, bias_two, kernel_two):
    inputs, rows, cols = latent.shape
    channels = kernel_in.shape[-1]
    count = lax.axis_size("rows")
    own = jnp.transpose(latent, (1, 0, 2))
    down = [(i, i + 1) for i in range(count - 1)]
    up = [(i + 1, i) for i in range(count - 1)]
    prev = lax.ppermute(own[rows - HALO :], "rows", down)
    after = lax.ppermute(own[:HALO], "rows", up)
    at = lax.axis_index("rows")
    edge = jnp.stack([at > 0, at < count - 1]).astype(jnp.int32)
    w_in = kernel_in.reshape(9 * inputs, channels)
    w_one = kernel_one.reshape(9 * channels, channels)
    w_two = kernel_two.reshape(9 * channels, channels)
    gain_one, bias_one, gain_two, bias_two = (v[None, :] for v in (gain_one, bias_one, gain_two, bias_two))

    def field(n):
        return jax.ShapeDtypeStruct((n, cols, channels), jnp.bfloat16)

    line = jax.ShapeDtypeStruct((count, LANES), jnp.float32)

    def patches(n):
        return pltpu.VMEM((n * 3 * inputs, cols), jnp.bfloat16)

    def cells(n):
        return pltpu.VMEM((n * cols, 3 * channels), jnp.bfloat16)

    row_flops = 2 * cols * channels * channels * 9
    partial = jax.ShapeDtypeStruct((2, channels), jnp.float32)
    inner, sums = call(inner_features, (field(rows - 2), partial), [patches(rows)], (own, w_in), row_flops, 16)
    latents = (prev, own, after, w_in)
    outer, moments = call(outer_features, (field(2), line), [patches(6)], (*latents, sums), row_flops, 16)
    gathered = over_all(moments, "rows")
    halo = call(halo_features, field(4), [patches(8)], latents, row_flops, 16)

    smem = pl.BlockSpec(memory_space=pltpu.SMEM)
    vmem = pl.BlockSpec(memory_space=pltpu.VMEM)
    away = pl.BlockSpec(memory_space=pl.ANY)
    parts = (edge, inner, outer, halo, gathered, gain_one, bias_one, w_one)
    weight = pltpu.VMEM((9 * channels, channels), jnp.bfloat16)
    stage = pltpu.VMEM((rows, cols, channels), jnp.bfloat16)
    three, six = pltpu.SemaphoreType.DMA((3,)), pltpu.SemaphoreType.DMA((rows,))
    first_specs = [smem] + [vmem] * 6 + [away]
    hidden, moments = call(
        own_hidden,
        (field(rows), line),
        [cells(rows + 2), weight, stage, three, six],
        parts,
        rows * row_flops,
        50,
        first_specs,
        (away, vmem),
    )
    gathered_two = over_all(moments, "rows")
    hidden_halo = call(halo_hidden, field(2), [cells(6), weight, three], parts, 2 * row_flops, 50, first_specs)
    return call(
        residual,
        field(rows),
        [cells(rows + 2), weight, stage, stage, three, six, six],
        (edge, pltpu.with_memory_space_constraint(hidden, pltpu.HBM), hidden_halo, inner, outer, gathered_two, gain_two, bias_two, w_two),
        rows * row_flops,
        50,
        [smem, away] + [vmem] * 6 + [away],
        away,
    )


def solution(mesh):
    in_specs = (P(None, ("batch", "rows"), None), P(), P(), P(), P(), P(), P(), P())
    out_specs = P(("batch", "rows"), None, None)
    return jax.shard_map(local, mesh=mesh, in_specs=in_specs, out_specs=out_specs, check_vma=False)
```

```python
import jax
import jax.numpy as jnp
from jax import lax
from jax.experimental import pallas as pl
from jax.experimental.pallas import tpu as pltpu
from jax.sharding import PartitionSpec as P

GROUPS = 32
EPSILON = 1e-06
LANES = 128
HALO = 3
BURSTS = (3, 5)


def dot(a, b):
    return jnp.dot(a, b, preferred_element_type=jnp.float32)


def split(values):
    high = values.astype(jnp.bfloat16).astype(jnp.float32)
    rest = values - high
    middle = rest.astype(jnp.bfloat16).astype(jnp.float32)
    return [high, middle, rest - middle]


def partial_sums(values):
    cells, channels = values.shape
    return jnp.sum(values.reshape(cells // 8, 8, channels), axis=0)


def store_moments(out_ref, sums, squares):
    channels = sums.shape[-1]
    channel = lax.broadcasted_iota(jnp.int32, (channels, LANES), 0)
    lane = lax.broadcasted_iota(jnp.int32, (channels, LANES), 1)
    member = (channel // (channels // GROUPS) == lane % GROUPS).astype(jnp.bfloat16)
    terms = jnp.concatenate(split(sums) + split(squares), axis=0).astype(jnp.bfloat16)
    totals = dot(terms, member)
    half = totals.shape[0] // 2
    first = jnp.sum(totals[:half], axis=0, keepdims=True)
    second = jnp.sum(totals[half:], axis=0, keepdims=True)
    line = jnp.where(lax.broadcasted_iota(jnp.int32, (8, LANES), 1) < GROUPS, first, second)
    for at in range(0, out_ref.shape[0], 8):
        out_ref[pl.ds(at, 8), :] = line


def half_affine(all_ref, gain_ref, bias_ref, cells):
    channels = gain_ref.shape[-1]
    count = cells * (channels // GROUPS) * all_ref.shape[0]
    channel = lax.broadcasted_iota(jnp.int32, (LANES, channels), 1) // (channels // GROUPS)
    lane = lax.broadcasted_iota(jnp.int32, (LANES, channels), 0)
    terms = jnp.concatenate(split(partial_sums(all_ref[...])), axis=0).astype(jnp.bfloat16)

    def mean(offset):
        member = (channel + offset == lane).astype(jnp.bfloat16)
        return jnp.sum(dot(terms, member), axis=0, keepdims=True) / count

    center, square = mean(0), mean(GROUPS)
    spread = jnp.maximum(square - center * center, 0.0)
    scale = lax.rsqrt(spread + EPSILON) * gain_ref[...]
    shift = bias_ref[...] - center * scale
    return scale * 0.5, shift * 0.5


def activate_row(value, scale, shift, inside, x_ref, slot):
    cols, channels = value.shape
    half = value.astype(jnp.float32) * scale + shift
    act = half * jnp.tanh(half) + half
    if inside is not None:
        act = jnp.where(inside, act, 0.0)
    zero = jnp.zeros((1, channels), jnp.float32)
    rows = pl.ds(slot * cols, cols)
    x_ref[rows, 0:channels] = jnp.concatenate([zero, act[:-1]], axis=0).astype(jnp.bfloat16)
    x_ref[rows, channels : 2 * channels] = act.astype(jnp.bfloat16)
    x_ref[rows, 2 * channels :] = jnp.concatenate([act[1:], zero], axis=0).astype(jnp.bfloat16)


def conv_row(x_ref, slot, weight_ref, cols):
    parts = [x_ref[pl.ds((slot + a) * cols, cols), :] for a in range(3)]
    return dot(jnp.concatenate(parts, axis=1), weight_ref[...])


def fill_patches(patch_ref, at, row):
    inputs, cols = row.shape
    values = row.astype(jnp.float32)
    lane = lax.broadcasted_iota(jnp.int32, values.shape, 1)
    left = jnp.where(lane == 0, 0.0, pltpu.roll(values, 1, 1))
    right = jnp.where(lane == cols - 1, 0.0, pltpu.roll(values, cols - 1, 1))
    for b, moved in enumerate((left, values, right)):
        patch_ref[pl.ds((3 * at + b) * inputs, inputs), :] = moved.astype(jnp.bfloat16)


def feature_row(patch_ref, at, inputs, weight):
    patch = patch_ref[pl.ds(3 * at * inputs, 9 * inputs), :]
    return lax.dot_general(patch, weight, (((0,), (0,)), ((), ())), preferred_element_type=jnp.float32).astype(jnp.bfloat16)


def feature_rows(patch_ref, spots, inputs, weight, out_ref):
    sums = squares = 0.0
    for r, at in enumerate(spots):
        rounded = feature_row(patch_ref, at, inputs, weight)
        out_ref[r] = rounded
        values = rounded.astype(jnp.float32)
        sums = sums + partial_sums(values)
        squares = squares + partial_sums(values * values)
    return sums, squares


def inner_features(own_ref, weight_ref, out_ref, sums_ref, patch_ref):
    rows, inputs, _ = own_ref.shape
    for at in range(rows):
        fill_patches(patch_ref, at, own_ref[at])
    sums, squares = feature_rows(patch_ref, range(rows - 2), inputs, weight_ref[...], out_ref)
    sums_ref[0] = sums
    sums_ref[1] = squares


def outer_features(prev_ref, own_ref, next_ref, weight_ref, sums_ref, out_ref, moments_ref, patch_ref):
    rows, inputs, _ = own_ref.shape
    lines = [prev_ref[HALO - 1], own_ref[0], own_ref[1], own_ref[rows - 2], own_ref[rows - 1], next_ref[0]]
    for at, line in enumerate(lines):
        fill_patches(patch_ref, at, line)
    sums, squares = feature_rows(patch_ref, (0, 3), inputs, weight_ref[...], out_ref)
    store_moments(moments_ref, sums + sums_ref[0], squares + sums_ref[1])


def halo_features(prev_ref, own_ref, next_ref, weight_ref, out_ref, patch_ref):
    rows, inputs, _ = own_ref.shape
    lines = [prev_ref[r] for r in range(3)] + [own_ref[0], own_ref[rows - 1]] + [next_ref[r] for r in range(3)]
    for at, line in enumerate(lines):
        fill_patches(patch_ref, at, line)
    weight = weight_ref[...]
    for r, at in enumerate((0, 1, 4, 5)):
        out_ref[r] = feature_row(patch_ref, at, inputs, weight)


def weight_copies(source_ref, weight_ref, sems):
    depth = weight_ref.shape[0] // 3
    return [
        pltpu.make_async_copy(source_ref.at[pl.ds(a * depth, depth)], weight_ref.at[pl.ds(a * depth, depth)], sems.at[a])
        for a in range(3)
    ]


def first_conv_row(x_ref, slot, weight_ref, cols, copies):
    depth = weight_ref.shape[0] // 3
    total = 0.0
    for a, copy in enumerate(copies):
        copy.wait()
        total = total + dot(x_ref[pl.ds((slot + a) * cols, cols), :], weight_ref[pl.ds(a * depth, depth), :])
    return total


def start_rows(stage_ref, out_ref, sems, first, end):
    copies = [pltpu.make_async_copy(stage_ref.at[r], out_ref.at[r], sems.at[r]) for r in range(first, end)]
    for copy in copies:
        copy.start()
    return copies


def feature_at(inner_ref, outer_ref, r):
    last = inner_ref.shape[0] + 1
    return outer_ref[r // last] if r in (0, last) else inner_ref[r - 1]


def own_hidden(
    edge_ref, inner_ref, outer_ref, halo_ref, all_ref, gain_ref, bias_ref, source_ref, out_ref, moments_ref,
    x_ref, weight_ref, stage_ref, weight_sems, sems,
):
    rows, cols = inner_ref.shape[0] + 2, inner_ref.shape[1]
    weights = weight_copies(source_ref, weight_ref, weight_sems)
    for copy in weights:
        copy.start()
    scale, shift = half_affine(all_ref, gain_ref, bias_ref, rows * cols)
    sums = squares = 0.0

    def fill(slot):
        if slot == 0:
            activate_row(halo_ref[1], scale, shift, edge_ref[0] > 0, x_ref, slot)
        elif slot == rows + 1:
            activate_row(halo_ref[2], scale, shift, edge_ref[1] > 0, x_ref, slot)
        else:
            activate_row(feature_at(inner_ref, outer_ref, slot - 1), scale, shift, None, x_ref, slot)

    for slot in range(3):
        fill(slot)
    copies = []
    for r in range(rows):
        if r:
            fill(r + 2)
        total = conv_row(x_ref, r, weight_ref, cols) if r else first_conv_row(x_ref, r, weight_ref, cols, weights)
        rounded = total.astype(jnp.bfloat16)
        stage_ref[r] = rounded
        values = rounded.astype(jnp.float32)
        sums = sums + partial_sums(values)
        squares = squares + partial_sums(values * values)
        if r in BURSTS:
            copies += start_rows(stage_ref, out_ref, sems, len(copies), r + 1)
    store_moments(moments_ref, sums, squares)
    for copy in copies:
        copy.wait()


def halo_hidden(
    edge_ref, inner_ref, outer_ref, halo_ref, all_ref, gain_ref, bias_ref, source_ref, out_ref, x_ref, weight_ref, weight_sems
):
    rows, cols = inner_ref.shape[0] + 2, inner_ref.shape[1]
    weights = weight_copies(source_ref, weight_ref, weight_sems)
    for copy in weights:
        copy.start()
    scale, shift = half_affine(all_ref, gain_ref, bias_ref, rows * cols)
    above, below = edge_ref[0] > 0, edge_ref[1] > 0
    activate_row(halo_ref[0], scale, shift, above, x_ref, 0)
    activate_row(halo_ref[1], scale, shift, above, x_ref, 1)
    activate_row(outer_ref[0], scale, shift, None, x_ref, 2)
    out_ref[0] = first_conv_row(x_ref, 0, weight_ref, cols, weights).astype(jnp.bfloat16)
    activate_row(outer_ref[1], scale, shift, None, x_ref, 3)
    activate_row(halo_ref[2], scale, shift, below, x_ref, 4)
    activate_row(halo_ref[3], scale, shift, below, x_ref, 5)
    out_ref[1] = conv_row(x_ref, 3, weight_ref, cols).astype(jnp.bfloat16)


def residual(
    edge_ref, hidden_ref, halo_ref, inner_ref, outer_ref, all_ref, gain_ref, bias_ref, source_ref, out_ref,
    x_ref, weight_ref, own_ref, stage_ref, weight_sems, own_sems, sems,
):
    rows, cols = inner_ref.shape[0] + 2, inner_ref.shape[1]
    loads = [pltpu.make_async_copy(hidden_ref.at[r], own_ref.at[r], own_sems.at[r]) for r in range(rows)]
    weights = weight_copies(source_ref, weight_ref, weight_sems)
    for copy in loads[:2] + weights + loads[2:]:
        copy.start()
    scale, shift = half_affine(all_ref, gain_ref, bias_ref, rows * cols)

    def fill(slot):
        if slot == 0:
            activate_row(halo_ref[0], scale, shift, edge_ref[0] > 0, x_ref, slot)
        elif slot == rows + 1:
            activate_row(halo_ref[1], scale, shift, edge_ref[1] > 0, x_ref, slot)
        else:
            activate_row(own_ref[slot - 1], scale, shift, None, x_ref, slot)

    loads[0].wait()
    loads[1].wait()
    for slot in range(3):
        fill(slot)
    copies = []
    for r in range(rows):
        if r == 1:
            for copy in loads[2:]:
                copy.wait()
        if r:
            fill(r + 2)
        total = conv_row(x_ref, r, weight_ref, cols) if r else first_conv_row(x_ref, r, weight_ref, cols, weights)
        total = feature_at(inner_ref, outer_ref, r).astype(jnp.float32) + total
        stage_ref[r] = total.astype(jnp.bfloat16)
        if r in BURSTS:
            copies += start_rows(stage_ref, out_ref, sems, len(copies), r + 1)
    for copy in copies:
        copy.wait()


def call(body, outs, scratch, operands, flops, limit, specs=None, out_specs=None):
    vmem = pl.BlockSpec(memory_space=pltpu.VMEM)
    return pl.pallas_call(
        body,
        out_shape=outs,
        in_specs=specs or [vmem] * len(operands),
        out_specs=out_specs or jax.tree.map(lambda _: vmem, outs),
        scratch_shapes=scratch,
        cost_estimate=pl.CostEstimate(flops=flops, transcendentals=0, bytes_accessed=1 << 20),
        compiler_params=pltpu.CompilerParams(vmem_limit_bytes=limit << 20),
    )(*operands)


def over_all(moments, axis):
    spread = lax.all_to_all(moments[:, None, :], axis, split_axis=0, concat_axis=0, tiled=True)
    return spread[:, 0, :]


def local(latent, kernel_in, gain_one, bias_one, kernel_one, gain_two, bias_two, kernel_two):
    inputs, rows, cols = latent.shape
    channels = kernel_in.shape[-1]
    count = lax.axis_size("rows")
    own = jnp.transpose(latent, (1, 0, 2))
    down = [(i, i + 1) for i in range(count - 1)]
    up = [(i + 1, i) for i in range(count - 1)]
    prev = lax.ppermute(own[rows - HALO :], "rows", down)
    after = lax.ppermute(own[:HALO], "rows", up)
    at = lax.axis_index("rows")
    edge = jnp.stack([at > 0, at < count - 1]).astype(jnp.int32)
    w_in = kernel_in.reshape(9 * inputs, channels)
    w_one = kernel_one.reshape(9 * channels, channels)
    w_two = kernel_two.reshape(9 * channels, channels)
    gain_one, bias_one, gain_two, bias_two = (v[None, :] for v in (gain_one, bias_one, gain_two, bias_two))

    def field(n):
        return jax.ShapeDtypeStruct((n, cols, channels), jnp.bfloat16)

    line = jax.ShapeDtypeStruct((count, LANES), jnp.float32)

    def patches(n):
        return pltpu.VMEM((n * 3 * inputs, cols), jnp.bfloat16)

    def cells(n):
        return pltpu.VMEM((n * cols, 3 * channels), jnp.bfloat16)

    row_flops = 2 * cols * channels * channels * 9
    partial = jax.ShapeDtypeStruct((2, 8, channels), jnp.float32)
    inner, sums = call(inner_features, (field(rows - 2), partial), [patches(rows)], (own, w_in), row_flops, 16)
    latents = (prev, own, after, w_in)
    outer, moments = call(outer_features, (field(2), line), [patches(6)], (*latents, sums), row_flops, 16)
    gathered = over_all(moments, "rows")
    halo = call(halo_features, field(4), [patches(8)], latents, row_flops, 16)

    smem = pl.BlockSpec(memory_space=pltpu.SMEM)
    vmem = pl.BlockSpec(memory_space=pltpu.VMEM)
    away = pl.BlockSpec(memory_space=pl.ANY)
    parts = (edge, inner, outer, halo, gathered, gain_one, bias_one, w_one)
    weight = pltpu.VMEM((9 * channels, channels), jnp.bfloat16)
    stage = pltpu.VMEM((rows, cols, channels), jnp.bfloat16)
    three, six = pltpu.SemaphoreType.DMA((3,)), pltpu.SemaphoreType.DMA((rows,))
    first_specs = [smem] + [vmem] * 6 + [away]
    hidden, moments = call(
        own_hidden,
        (field(rows), line),
        [cells(rows + 2), weight, stage, three, six],
        parts,
        rows * row_flops,
        50,
        first_specs,
        (away, vmem),
    )
    gathered_two = over_all(moments, "rows")
    hidden_halo = call(halo_hidden, field(2), [cells(6), weight, three], parts, 2 * row_flops, 50, first_specs)
    return call(
        residual,
        field(rows),
        [cells(rows + 2), weight, stage, stage, three, six, six],
        (edge, pltpu.with_memory_space_constraint(hidden, pltpu.HBM), hidden_halo, inner, outer, gathered_two, gain_two, bias_two, w_two),
        rows * row_flops,
        50,
        [smem, away] + [vmem] * 6 + [away],
        away,
    )


def solution(mesh):
    in_specs = (P(None, ("batch", "rows"), None), P(), P(), P(), P(), P(), P(), P())
    out_specs = P(("batch", "rows"), None, None)
    return jax.shard_map(local, mesh=mesh, in_specs=in_specs, out_specs=out_specs, check_vma=False)
```

```python
import jax
import jax.numpy as jnp
from jax import lax
from jax.experimental import pallas as pl
from jax.experimental.pallas import tpu as pltpu
from jax.sharding import PartitionSpec as P

GROUPS = 32
EPSILON = 1e-06
LANES = 128
HALO = 3
BURSTS = (3, 5)


def dot(a, b):
    return jnp.dot(a, b, preferred_element_type=jnp.float32)


def split(values):
    high = values.astype(jnp.bfloat16).astype(jnp.float32)
    rest = values - high
    middle = rest.astype(jnp.bfloat16).astype(jnp.float32)
    return [high, middle, rest - middle]


def partial_sums(values):
    cells, channels = values.shape
    return jnp.sum(values.reshape(cells // 8, 8, channels), axis=0)


def store_moments(out_ref, sums, squares):
    channels = sums.shape[-1]
    channel = lax.broadcasted_iota(jnp.int32, (channels, LANES), 0)
    lane = lax.broadcasted_iota(jnp.int32, (channels, LANES), 1)
    member = (channel // (channels // GROUPS) == lane % GROUPS).astype(jnp.bfloat16)
    terms = jnp.concatenate(split(sums) + split(squares), axis=0).astype(jnp.bfloat16)
    totals = dot(terms, member)
    half = totals.shape[0] // 2
    first = jnp.sum(totals[:half], axis=0, keepdims=True)
    second = jnp.sum(totals[half:], axis=0, keepdims=True)
    line = jnp.where(lax.broadcasted_iota(jnp.int32, (8, LANES), 1) < GROUPS, first, second)
    for at in range(0, out_ref.shape[0], 8):
        out_ref[pl.ds(at, 8), :] = line


def half_affine(all_ref, gain_ref, bias_ref, cells):
    channels = gain_ref.shape[-1]
    count = cells * (channels // GROUPS) * all_ref.shape[0]
    channel = lax.broadcasted_iota(jnp.int32, (LANES, channels), 1) // (channels // GROUPS)
    lane = lax.broadcasted_iota(jnp.int32, (LANES, channels), 0)
    terms = jnp.concatenate(split(partial_sums(all_ref[...])), axis=0).astype(jnp.bfloat16)

    def mean(offset):
        member = (channel + offset == lane).astype(jnp.bfloat16)
        return jnp.sum(dot(terms, member), axis=0, keepdims=True) / count

    center, square = mean(0), mean(GROUPS)
    spread = jnp.maximum(square - center * center, 0.0)
    scale = lax.rsqrt(spread + EPSILON) * gain_ref[...]
    shift = bias_ref[...] - center * scale
    return scale * 0.5, shift * 0.5


def activate_row(value, scale, shift, inside, x_ref, slot):
    cols, channels = value.shape
    half = value.astype(jnp.float32) * scale + shift
    act = half * jnp.tanh(half) + half
    if inside is not None:
        act = jnp.where(inside, act, 0.0)
    zero = jnp.zeros((1, channels), jnp.float32)
    rows = pl.ds(slot * cols, cols)
    x_ref[rows, 0:channels] = jnp.concatenate([zero, act[:-1]], axis=0).astype(jnp.bfloat16)
    x_ref[rows, channels : 2 * channels] = act.astype(jnp.bfloat16)
    x_ref[rows, 2 * channels :] = jnp.concatenate([act[1:], zero], axis=0).astype(jnp.bfloat16)


def conv_row(x_ref, slot, weight_ref, cols):
    parts = [x_ref[pl.ds((slot + a) * cols, cols), :] for a in range(3)]
    return dot(jnp.concatenate(parts, axis=1), weight_ref[...])


def fill_patches(patch_ref, at, row):
    inputs, cols = row.shape
    values = row.astype(jnp.float32)
    lane = lax.broadcasted_iota(jnp.int32, values.shape, 1)
    left = jnp.where(lane == 0, 0.0, pltpu.roll(values, 1, 1))
    right = jnp.where(lane == cols - 1, 0.0, pltpu.roll(values, cols - 1, 1))
    for b, moved in enumerate((left, values, right)):
        patch_ref[pl.ds((3 * at + b) * inputs, inputs), :] = moved.astype(jnp.bfloat16)


def feature_row(patch_ref, at, inputs, weight):
    patch = patch_ref[pl.ds(3 * at * inputs, 9 * inputs), :]
    return lax.dot_general(patch, weight, (((0,), (0,)), ((), ())), preferred_element_type=jnp.float32).astype(jnp.bfloat16)


def feature_rows(patch_ref, spots, inputs, weight, out_ref):
    sums = squares = 0.0
    for r, at in enumerate(spots):
        rounded = feature_row(patch_ref, at, inputs, weight)
        out_ref[r] = rounded
        values = rounded.astype(jnp.float32)
        sums = sums + partial_sums(values)
        squares = squares + partial_sums(values * values)
    return sums, squares


def inner_features(own_ref, weight_ref, out_ref, sums_ref, patch_ref):
    rows, inputs, _ = own_ref.shape
    for at in range(rows):
        fill_patches(patch_ref, at, own_ref[at])
    sums, squares = feature_rows(patch_ref, range(rows - 2), inputs, weight_ref[...], out_ref)
    sums_ref[0] = sums
    sums_ref[1] = squares


def outer_features(prev_ref, own_ref, next_ref, weight_ref, sums_ref, out_ref, moments_ref, patch_ref):
    rows, inputs, _ = own_ref.shape
    lines = [prev_ref[HALO - 1], own_ref[0], own_ref[1], own_ref[rows - 2], own_ref[rows - 1], next_ref[0]]
    for at, line in enumerate(lines):
        fill_patches(patch_ref, at, line)
    sums, squares = feature_rows(patch_ref, (0, 3), inputs, weight_ref[...], out_ref)
    store_moments(moments_ref, sums + sums_ref[0], squares + sums_ref[1])


def halo_features(prev_ref, own_ref, next_ref, weight_ref, out_ref, patch_ref):
    rows, inputs, _ = own_ref.shape
    lines = [prev_ref[r] for r in range(3)] + [own_ref[0], own_ref[rows - 1]] + [next_ref[r] for r in range(3)]
    for at, line in enumerate(lines):
        fill_patches(patch_ref, at, line)
    weight = weight_ref[...]
    for r, at in enumerate((0, 1, 4, 5)):
        out_ref[r] = feature_row(patch_ref, at, inputs, weight)


def mixed_taps(taps_ref, _, out_ref):
    taps = [taps_ref[a].astype(jnp.float32) * 0.5 for a in range(3)]
    ends = taps[0] + taps[2]
    out_ref[0] = (ends + taps[1]).astype(jnp.bfloat16)
    out_ref[1] = (ends - taps[1]).astype(jnp.bfloat16)


def four_taps(source_ref, mixed_ref):
    depth = source_ref.shape[0] // 3
    return [source_ref.at[pl.ds(0, depth)], mixed_ref.at[0], mixed_ref.at[1], source_ref.at[pl.ds(2 * depth, depth)]]


def weight_copies(sources, weight_ref, sems):
    depth = weight_ref.shape[0] // len(sources)
    return [
        pltpu.make_async_copy(source, weight_ref.at[pl.ds(a * depth, depth)], sems.at[a]) for a, source in enumerate(sources)
    ]


def first_conv_row(x_ref, slot, weight_ref, cols, copies):
    depth = weight_ref.shape[0] // 3
    total = 0.0
    for a, copy in enumerate(copies):
        copy.wait()
        total = total + dot(x_ref[pl.ds((slot + a) * cols, cols), :], weight_ref[pl.ds(a * depth, depth), :])
    return total


def conv_pair(x_ref, slot, weight_ref, cols, copies, m_ref):
    depth = weight_ref.shape[0] // 4

    def product(k, sign, near, far):
        if copies:
            copies[k].wait()
        left = x_ref[pl.ds((slot + near) * cols, cols), :]
        right = x_ref[pl.ds((slot + far) * cols, cols), :]
        return dot(left + right if sign > 0 else left - right, weight_ref[pl.ds(k * depth, depth), :])

    for k, sign, near, far in ((0, -1, 0, 2), (1, 1, 1, 2), (2, -1, 2, 1), (3, -1, 1, 3)):
        m_ref[k] = product(k, sign, near, far)
    return m_ref[0] + m_ref[1] + m_ref[2], m_ref[1] - m_ref[2] - m_ref[3]


def start_rows(stage_ref, out_ref, sems, first, end):
    copies = [pltpu.make_async_copy(stage_ref.at[r], out_ref.at[r], sems.at[r]) for r in range(first, end)]
    for copy in copies:
        copy.start()
    return copies


def feature_at(inner_ref, outer_ref, r):
    last = inner_ref.shape[0] + 1
    return outer_ref[r // last] if r in (0, last) else inner_ref[r - 1]


def own_hidden(
    edge_ref, inner_ref, outer_ref, halo_ref, all_ref, gain_ref, bias_ref, source_ref, out_ref, moments_ref,
    x_ref, weight_ref, stage_ref, weight_sems, sems,
):
    rows, cols = inner_ref.shape[0] + 2, inner_ref.shape[1]
    depth = weight_ref.shape[0] // 3
    weights = weight_copies([source_ref.at[pl.ds(a * depth, depth)] for a in range(3)], weight_ref, weight_sems)
    for copy in weights:
        copy.start()
    scale, shift = half_affine(all_ref, gain_ref, bias_ref, rows * cols)
    sums = squares = 0.0

    def fill(slot):
        if slot == 0:
            activate_row(halo_ref[1], scale, shift, edge_ref[0] > 0, x_ref, slot)
        elif slot == rows + 1:
            activate_row(halo_ref[2], scale, shift, edge_ref[1] > 0, x_ref, slot)
        else:
            activate_row(feature_at(inner_ref, outer_ref, slot - 1), scale, shift, None, x_ref, slot)

    for slot in range(3):
        fill(slot)
    copies = []
    for r in range(rows):
        if r:
            fill(r + 2)
        total = conv_row(x_ref, r, weight_ref, cols) if r else first_conv_row(x_ref, r, weight_ref, cols, weights)
        rounded = total.astype(jnp.bfloat16)
        stage_ref[r] = rounded
        values = rounded.astype(jnp.float32)
        sums = sums + partial_sums(values)
        squares = squares + partial_sums(values * values)
        if r in BURSTS:
            copies += start_rows(stage_ref, out_ref, sems, len(copies), r + 1)
    store_moments(moments_ref, sums, squares)
    for copy in copies:
        copy.wait()


def halo_hidden(
    edge_ref, inner_ref, outer_ref, halo_ref, all_ref, gain_ref, bias_ref, source_ref, out_ref, x_ref, weight_ref, weight_sems
):
    rows, cols = inner_ref.shape[0] + 2, inner_ref.shape[1]
    depth = weight_ref.shape[0] // 3
    weights = weight_copies([source_ref.at[pl.ds(a * depth, depth)] for a in range(3)], weight_ref, weight_sems)
    for copy in weights:
        copy.start()
    scale, shift = half_affine(all_ref, gain_ref, bias_ref, rows * cols)
    above, below = edge_ref[0] > 0, edge_ref[1] > 0
    activate_row(halo_ref[0], scale, shift, above, x_ref, 0)
    activate_row(halo_ref[1], scale, shift, above, x_ref, 1)
    activate_row(outer_ref[0], scale, shift, None, x_ref, 2)
    out_ref[0] = first_conv_row(x_ref, 0, weight_ref, cols, weights).astype(jnp.bfloat16)
    activate_row(outer_ref[1], scale, shift, None, x_ref, 3)
    activate_row(halo_ref[2], scale, shift, below, x_ref, 4)
    activate_row(halo_ref[3], scale, shift, below, x_ref, 5)
    out_ref[1] = conv_row(x_ref, 3, weight_ref, cols).astype(jnp.bfloat16)


def residual(
    edge_ref, hidden_ref, halo_ref, inner_ref, outer_ref, all_ref, gain_ref, bias_ref, source_ref, mixed_ref, out_ref,
    x_ref, weight_ref, own_ref, stage_ref, m_ref, weight_sems, own_sems, sems,
):
    rows, cols = inner_ref.shape[0] + 2, inner_ref.shape[1]
    loads = [pltpu.make_async_copy(hidden_ref.at[r], own_ref.at[r], own_sems.at[r]) for r in range(rows)]
    weights = weight_copies(four_taps(source_ref, mixed_ref), weight_ref, weight_sems)
    for copy in loads[:3] + weights + loads[3:]:
        copy.start()
    scale, shift = half_affine(all_ref, gain_ref, bias_ref, rows * cols)

    def fill(slot):
        if slot == 0:
            activate_row(halo_ref[0], scale, shift, edge_ref[0] > 0, x_ref, slot)
        elif slot == rows + 1:
            activate_row(halo_ref[1], scale, shift, edge_ref[1] > 0, x_ref, slot)
        else:
            activate_row(own_ref[slot - 1], scale, shift, None, x_ref, slot)

    for copy in loads[:3]:
        copy.wait()
    fill(0)
    fill(1)
    copies = []
    for r in range(0, rows, 2):
        if r == 2:
            for copy in loads[3:]:
                copy.wait()
        fill(r + 2)
        fill(r + 3)
        for k, total in enumerate(conv_pair(x_ref, r, weight_ref, cols, [] if r else weights, m_ref)):
            total = feature_at(inner_ref, outer_ref, r + k).astype(jnp.float32) + total
            stage_ref[r + k] = total.astype(jnp.bfloat16)
        if r + 1 in BURSTS:
            copies += start_rows(stage_ref, out_ref, sems, len(copies), r + 2)
    for copy in copies:
        copy.wait()


def call(body, outs, scratch, operands, flops, limit, specs=None, out_specs=None):
    vmem = pl.BlockSpec(memory_space=pltpu.VMEM)
    return pl.pallas_call(
        body,
        out_shape=outs,
        in_specs=specs or [vmem] * len(operands),
        out_specs=out_specs or jax.tree.map(lambda _: vmem, outs),
        scratch_shapes=scratch,
        cost_estimate=pl.CostEstimate(flops=flops, transcendentals=0, bytes_accessed=1 << 20),
        compiler_params=pltpu.CompilerParams(vmem_limit_bytes=limit << 20),
    )(*operands)


def mixed(kernel, after):
    depth, channels = 3 * kernel.shape[-2], kernel.shape[-1]
    block = depth // 6
    return pl.pallas_call(
        mixed_taps,
        out_shape=jax.ShapeDtypeStruct((2, depth, channels), jnp.bfloat16),
        grid=(6,),
        in_specs=[
            pl.BlockSpec((3, block, channels), lambda i: (0, i, 0)),
            pl.BlockSpec(memory_space=pl.ANY),
        ],
        out_specs=pl.BlockSpec((2, block, channels), lambda i: (0, i, 0)),
        cost_estimate=pl.CostEstimate(flops=1 << 31, transcendentals=0, bytes_accessed=8 << 20),
        compiler_params=pltpu.CompilerParams(vmem_limit_bytes=50 << 20),
    )(kernel.reshape(3, depth, channels), after)


def over_all(moments, axis):
    spread = lax.all_to_all(moments[:, None, :], axis, split_axis=0, concat_axis=0, tiled=True)
    return spread[:, 0, :]


def local(latent, kernel_in, gain_one, bias_one, kernel_one, gain_two, bias_two, kernel_two):
    inputs, rows, cols = latent.shape
    channels = kernel_in.shape[-1]
    count = lax.axis_size("rows")
    own = jnp.transpose(latent, (1, 0, 2))
    down = [(i, i + 1) for i in range(count - 1)]
    up = [(i + 1, i) for i in range(count - 1)]
    prev = lax.ppermute(own[rows - HALO :], "rows", down)
    after = lax.ppermute(own[:HALO], "rows", up)
    at = lax.axis_index("rows")
    edge = jnp.stack([at > 0, at < count - 1]).astype(jnp.int32)
    w_in = kernel_in.reshape(9 * inputs, channels)
    w_one = kernel_one.reshape(9 * channels, channels)
    w_two = kernel_two.reshape(9 * channels, channels)
    gain_one, bias_one, gain_two, bias_two = (v[None, :] for v in (gain_one, bias_one, gain_two, bias_two))

    def field(n):
        return jax.ShapeDtypeStruct((n, cols, channels), jnp.bfloat16)

    line = jax.ShapeDtypeStruct((count, LANES), jnp.float32)

    def patches(n):
        return pltpu.VMEM((n * 3 * inputs, cols), jnp.bfloat16)

    def cells(n):
        return pltpu.VMEM((n * cols, 3 * channels), jnp.bfloat16)

    row_flops = 2 * cols * channels * channels * 9
    partial = jax.ShapeDtypeStruct((2, 8, channels), jnp.float32)
    inner, sums = call(inner_features, (field(rows - 2), partial), [patches(rows)], (own, w_in), row_flops, 16)
    latents = (prev, own, after, w_in)
    outer, moments = call(outer_features, (field(2), line), [patches(6)], (*latents, sums), row_flops, 16)
    gathered = over_all(moments, "rows")
    halo = call(halo_features, field(4), [patches(8)], latents, row_flops, 16)

    smem = pl.BlockSpec(memory_space=pltpu.SMEM)
    vmem = pl.BlockSpec(memory_space=pltpu.VMEM)
    away = pl.BlockSpec(memory_space=pl.ANY)
    parts = (edge, inner, outer, halo, gathered, gain_one, bias_one, w_one)
    weight = pltpu.VMEM((9 * channels, channels), jnp.bfloat16)
    stage = pltpu.VMEM((rows, cols, channels), jnp.bfloat16)
    four_weights = pltpu.VMEM((12 * channels, channels), jnp.bfloat16)
    products = pltpu.VMEM((4, cols, channels), jnp.float32)
    four = pltpu.SemaphoreType.DMA((4,))
    three, six = pltpu.SemaphoreType.DMA((3,)), pltpu.SemaphoreType.DMA((rows,))
    first_specs = [smem] + [vmem] * 6 + [away]
    hidden, moments = call(
        own_hidden,
        (field(rows), line),
        [cells(rows + 2), weight, stage, three, six],
        parts,
        rows * row_flops,
        50,
        first_specs,
        (away, vmem),
    )
    gathered_two = over_all(moments, "rows")
    hidden_halo = call(halo_hidden, field(2), [cells(6), weight, three], parts, 2 * row_flops, 50, first_specs)
    mixed_two = mixed(kernel_two, hidden_halo)
    return call(
        residual,
        field(rows),
        [cells(rows + 2), four_weights, stage, stage, products, four, six, six],
        (edge, pltpu.with_memory_space_constraint(hidden, pltpu.HBM), hidden_halo, inner, outer, gathered_two, gain_two, bias_two, w_two, mixed_two),
        rows * row_flops,
        50,
        [smem, away] + [vmem] * 6 + [away] * 2,
        away,
    )


def solution(mesh):
    in_specs = (P(None, ("batch", "rows"), None), P(), P(), P(), P(), P(), P(), P())
    out_specs = P(("batch", "rows"), None, None)
    return jax.shard_map(local, mesh=mesh, in_specs=in_specs, out_specs=out_specs, check_vma=False)
```
